32 devices in a mesh: prompt: 4 (over y, x), sample: 8 (over z, core).
Axes of the slice: x: 2, y: 2, z: 4, core: 2. Of those that a mesh axis runs over, the one named last changes fastest.
Arguments:
- queries: bfloat16 [4, 64, 4096], P('prompt', 'sample'), may hold values from -250 to 250
- prompt_cache: bfloat16 [4, 8, 2048, 2048], P('prompt', 'sample'), may hold values from -6 to 6
- owner: int32 [4], P('prompt'), may hold values from 0 to 7
- prompt_len: int32 [4], P('prompt'), may hold values from 512 to 2048
- suffix_cache: bfloat16 [4, 64, 256, 2048], P('prompt', 'sample'), may hold values from -6 to 6
- suffix_len: int32 [4, 64], P('prompt', 'sample'), may hold values from 1 to 256
- new_kv: bfloat16 [4, 64, 2048], P('prompt', 'sample'), may hold values from -6 to 6
- out_weight: bfloat16 [4096, 4096], P(None, 'sample'), may hold values from -0.09375 to 0.09375
Outputs:
- mixed: bfloat16 [4, 64, 4096], P('prompt', None, 'sample')
The draws below stay inside these ranges and needn't reach their ends.
All inputs are finite; a program needn't handle non-finite values.
Results may differ from the reference program's by a relative error of at most 0.007.
Values may be sent and summed in bfloat16 or wider, within the bound.
A program may use at most 192 MiB of HBM per device.

```python
import jax
import jax.numpy as jnp
from jax import lax

D = 4096
H = 32
KVH = 8
HD = 128
PLEN = 2048
SLEN = 256
PROMPTS = 4
SLOTS = 8
SAMPLES = 64
QW = 4096
KV2 = 2048
N_SAMPLE = 8


def shared_draw(key):
    key_cache, key_query = jax.random.split(jax.random.fold_in(key, 7))
    cache = jnp.clip(jax.random.normal(key_cache, (PROMPTS, SLOTS, PLEN, KV2), jnp.float32), -6.0, 6.0)
    queries = 0.5 * jnp.clip(jax.random.normal(key_query, (PROMPTS, SAMPLES, H * HD), jnp.float32), -6.0, 6.0)
    return (cache, queries)


def draw_queries(key, part):
    return shared_draw(key)[1].astype(jnp.bfloat16)


def draw_prompt_cache(key, part):
    return shared_draw(key)[0].astype(jnp.bfloat16)


def with_ends(values, rng, smallest, high):
    shape = values.shape
    spot = [jax.random.randint(jax.random.fold_in(rng, axis), (), 0, shape[axis]) for axis in range(len(shape))]
    values = values.at[tuple(spot)].set(smallest)
    longest = shape.index(max(shape))
    spot[longest] = (spot[longest] + 1) % shape[longest]
    return values.at[tuple(spot)].set(high)


def shard_levels(key, shape, cuts, smallest, largest):
    gain = 1.0
    for dim, blocks in cuts:
        steps = jax.random.uniform(jax.random.fold_in(jax.random.fold_in(key, 6), dim), (blocks,), jnp.float32, smallest / len(cuts), largest / len(cuts))
        gain = gain * jnp.repeat(jnp.exp(steps), shape[dim] // blocks).reshape((-1,) + (1,) * (len(shape) - 1 - dim))
    return gain


def noise(rng, shape, deviation, reach, cuts=(), kind=jnp.bfloat16):
    result = deviation * jax.random.normal(rng, shape, jnp.float32)
    if cuts:
        result = result * shard_levels(rng, shape, cuts, -0.22, 0.18)
    return jnp.clip(result, -reach, reach).astype(kind)


def setup_inputs(seed: int = 0) -> dict:
    streams_of = jax.random.split(jax.random.key(seed), 9)
    queries = draw_queries(jax.random.fold_in(streams_of[8], 71), 0)
    prompt_cache = draw_prompt_cache(jax.random.fold_in(streams_of[8], 71), 0)
    owner = with_ends(jax.random.randint(streams_of[2], (PROMPTS,), 0, N_SAMPLE), jax.random.fold_in(streams_of[2], 1), 0, N_SAMPLE - 1).astype(jnp.int32)
    prompt_len = with_ends(jax.random.randint(streams_of[3], (PROMPTS,), PLEN // 4, PLEN + 1), jax.random.fold_in(streams_of[3], 1), PLEN // 4, PLEN).astype(jnp.int32)
    suffix_cache = noise(streams_of[4], (PROMPTS, SAMPLES, SLEN, KV2), 1.0, 6.0, ((0, 4), (1, 8)))
    suffix_len = with_ends(jax.random.randint(streams_of[5], (PROMPTS, SAMPLES), 1, SLEN + 1), jax.random.fold_in(streams_of[5], 1), 1, SLEN).astype(jnp.int32)
    new_kv = noise(streams_of[6], (PROMPTS, SAMPLES, KV2), 1.0, 6.0, ((0, 4), (1, 8)))
    out_weight = noise(streams_of[7], (QW, D), QW ** -0.5, 0.09375, ((1, 8),))
    return {"queries": queries, "prompt_cache": prompt_cache, "owner": owner, "prompt_len": prompt_len, "suffix_cache": suffix_cache, "suffix_len": suffix_len, "new_kv": new_kv, "out_weight": out_weight}


def prefix_part(queries, cache, length):
    count = queries.shape[0]
    positions = cache.shape[0]
    query = queries.astype(jnp.float32).reshape(count, KVH, H // KVH, HD)
    keys = cache[:, :KVH * HD].astype(jnp.float32).reshape(positions, KVH, HD)
    values = cache[:, KVH * HD:].astype(jnp.float32).reshape(positions, KVH, HD)
    scores = jnp.einsum("sgjd,tgd->sgjt", query, keys) * (HD ** -0.5)
    valid = jnp.arange(positions, dtype=jnp.int32) < length
    scores = jnp.where(valid, scores, -1e30)
    top = jnp.max(scores, axis=-1)
    weights = jnp.exp(scores - top[..., None])
    total = jnp.sum(weights, axis=-1)
    rounded = weights.astype(jnp.bfloat16).astype(jnp.float32)
    output = jnp.einsum("sgjt,tgd->sgjd", rounded, values)
    return output.reshape(count, H, HD), top.reshape(count, H), total.reshape(count, H)


def suffix_part(queries, cache, lengths, own):
    count = queries.shape[0]
    positions = cache.shape[1]
    query = queries.astype(jnp.float32).reshape(count, KVH, H // KVH, HD)
    keys = cache[:, :, :KVH * HD].astype(jnp.float32).reshape(count, positions, KVH, HD)
    values = cache[:, :, KVH * HD:].astype(jnp.float32).reshape(count, positions, KVH, HD)
    own_key = own[:, :KVH * HD].astype(jnp.float32).reshape(count, KVH, HD)
    own_value = own[:, KVH * HD:].astype(jnp.float32).reshape(count, KVH, HD)
    scores = jnp.einsum("sgjd,stgd->sgjt", query, keys) * (HD ** -0.5)
    valid = jnp.arange(positions, dtype=jnp.int32)[None, :] < lengths[:, None]
    scores = jnp.where(valid[:, None, None, :], scores, -1e30)
    own_score = jnp.einsum("sgjd,sgd->sgj", query, own_key) * (HD ** -0.5)
    top = jnp.maximum(jnp.max(scores, axis=-1), own_score)
    weights = jnp.exp(scores - top[..., None])
    own_weight = jnp.exp(own_score - top)
    total = jnp.sum(weights, axis=-1) + own_weight
    rounded = weights.astype(jnp.bfloat16).astype(jnp.float32)
    output = jnp.einsum("sgjt,stgd->sgjd", rounded, values)
    own_rounded = own_weight.astype(jnp.bfloat16).astype(jnp.float32)
    output = output + own_rounded[..., None] * own_value[:, :, None, :]
    return output.reshape(count, H, HD), top.reshape(count, H), total.reshape(count, H)


def combine(prefix, suffix):
    out_pre, top_pre, total_pre = prefix
    out_suf, top_suf, total_suf = suffix
    top = jnp.maximum(top_pre, top_suf)
    factor_pre = jnp.exp(top_pre - top)
    factor_suf = jnp.exp(top_suf - top)
    numer = out_pre * factor_pre[..., None] + out_suf * factor_suf[..., None]
    denom = total_pre * factor_pre + total_suf * factor_suf
    attn = numer / denom[..., None]
    return attn.reshape(attn.shape[0], H * HD).astype(jnp.bfloat16)


def reference(queries, prompt_cache, owner, prompt_len, suffix_cache, suffix_len, new_kv, out_weight):
    def one_prompt(index):
        prefix = prefix_part(queries[index], prompt_cache[index, owner[index]], prompt_len[index])
        suffix = suffix_part(queries[index], suffix_cache[index], suffix_len[index], new_kv[index])
        attn = combine(prefix, suffix)
        return jnp.dot(attn, out_weight, preferred_element_type=jnp.float32).astype(jnp.bfloat16)

    return lax.map(one_prompt, jnp.arange(PROMPTS, dtype=jnp.int32))
```

```python
import functools

import jax
import jax.numpy as jnp
from jax import lax
from jax.experimental import pallas as pl
from jax.experimental.pallas import tpu as pltpu
from jax.sharding import PartitionSpec as P

H = 32
KVH = 8
HD = 128
GROUP = H // KVH
HALF_H = H // 2
HALF_G = KVH // 2
HALF_W = HALF_H * HD
KW = KVH * HD
GW = GROUP * HD
PAIRS = HALF_H // 2
PARCELS = ((0, 2), (2, 2), (4, 2), (6, 2), (8, 2), (10, 2), (12, 2), (14, 1), (15, 1))
EARLY = (4, 2)
FACTOR = HD ** (-0.5) * 1.4426950408889634
NEG = -1e30
F32 = jnp.float32
BF16 = jnp.bfloat16
NT = (((1,), (1,)), ((), ()))


def kernel(
    n,
    owner_hbm,
    plen_hbm,
    slen_hbm,
    q_hbm,
    new_hbm,
    cache_ref,
    suffix_ref,
    w_ref,
    out_ref,
    kv0,
    kv1,
    kv2,
    kv3,
    suf,
    wbuf,
    owner_ref,
    plen_ref,
    slen_ref,
    q_ref,
    new_ref,
    qall,
    qrow,
    orow,
    ssrc,
    sother,
    s16,
    lse_all,
    lse_src,
    lse_other,
    lse_suf,
    turned,
    scol,
    lse,
    padded,
    share,
    near_share,
    mine,
    arrived,
    leaving,
    attn,
    attn_in,
    acc,
    in_sem,
    suf_sem,
    kv_sem,
    w_sem,
    q_send,
    q_recv,
    s_send,
    s_recv,
    kv_send,
    kv_recv,
    lse_send,
    lse_recv,
    o_send,
    o_recv,
    a_send,
    a_recv,
):
    kv = (kv0, kv1, kv2, kv3)
    me = lax.axis_index("sample")
    chip = me // 2
    core = me % 2
    chips = n // 2
    partner = chip * 2 + (1 - core)
    count = q_ref.shape[0]
    total = n * count
    both = 2 * count
    span = 2 * total
    slen = suffix_ref.shape[2]
    near = chip // (chips // 2)
    at_end = (chip == 0) | (chip == chips - 1)
    inside = (chip > 0) & (chip < chips - 1)

    def remote(src, dst, send, recv, to):
        return pltpu.make_async_remote_copy(
            src_ref=src,
            dst_ref=dst,
            send_sem=send,
            recv_sem=recv,
            device_id={"sample": to},
            device_id_type=pl.DeviceIdType.MESH,
        )

    barrier = pltpu.get_barrier_semaphore()
    for d in range(1, n):
        pl.semaphore_signal(
            barrier,
            inc=1,
            device_id={"sample": (me + d) % n},
            device_id_type=pl.DeviceIdType.MESH,
        )

    q_in = pltpu.make_async_copy(q_hbm.at[0], q_ref, in_sem.at[0])
    new_in = pltpu.make_async_copy(new_hbm.at[0], new_ref, in_sem.at[1])
    slen_in = pltpu.make_async_copy(slen_hbm, slen_ref, in_sem.at[2])
    owner_in = pltpu.make_async_copy(owner_hbm, owner_ref, in_sem.at[3])
    plen_in = pltpu.make_async_copy(plen_hbm, plen_ref, in_sem.at[4])
    suf_copies = [
        pltpu.make_async_copy(suffix_ref.at[0, b], suf.at[b], suf_sem.at[b])
        for b in range(count)
    ]
    q_in.start()
    slen_in.start()
    new_in.start()
    for copy in suf_copies[:2]:
        copy.start()

    def kv_local(k, part):
        col = part * KW + (core * HALF_G + k) * HD
        return pltpu.make_async_copy(
            cache_ref.at[0, 0, :, pl.ds(pl.multiple_of(col, HD), HD)],
            kv[k].at[core, part],
            kv_sem.at[k],
        )

    def kv_remote(k, part):
        col = part * KW + ((1 - core) * HALF_G + k) * HD
        return remote(
            cache_ref.at[0, 0, :, pl.ds(pl.multiple_of(col, HD), HD)],
            kv[k].at[core, part],
            kv_send.at[k],
            kv_recv.at[k],
            partner,
        )

    def kv_wait(k):
        here = kv[k].at[core]
        pltpu.make_async_copy(here, here, kv_sem.at[k]).wait()
        there = kv[k].at[1 - core]
        remote(there, there, kv_send.at[k], kv_recv.at[k], partner).wait_recv()

    def w_copy(half):
        return pltpu.make_async_copy(
            w_ref.at[pl.ds(half * HALF_W, HALF_W), :], wbuf.at[half], w_sem.at[0]
        )

    padded[...] = jnp.zeros(padded.shape, F32)
    lse_all[...] = jnp.zeros(lse_all.shape, F32)
    q_in.wait()
    for copy in suf_copies[2:]:
        copy.start()
    q32 = q_ref[...].astype(F32)
    for h in range(H):
        qrow[h * count : (h + 1) * count, :] = q32[:, h * HD : (h + 1) * HD]
    new_in.wait()
    slen_in.wait()
    owner_in.start()
    plen_in.start()
    for k in range(HALF_G):
        for part in range(2):
            kv_local(k, part).start()
    for half in range(2):
        w_copy(half).start()
    new32 = new_ref[...].astype(F32)

    row_group = lax.broadcasted_iota(jnp.int32, (H, HD), 0) // GROUP
    lane = lax.broadcasted_iota(jnp.int32, (H, span), 1) - (total + me * count)
    pos = lax.broadcasted_iota(jnp.int32, (1, slen), 1)

    def suffix(first):
        batch = range(first, first + 2)
        spreads, own_scores = [], []
        for b in batch:
            query = qrow[pl.ds(b, H, stride=count), :]
            spread = jnp.concatenate(
                [jnp.where(row_group == g, query, 0.0) for g in range(KVH)], axis=1
            )
            own = spread * new32[b : b + 1, :KW]
            folded = own[:, :HD]
            for g in range(1, KVH):
                folded = folded + own[:, g * HD : (g + 1) * HD]
            own_scores.append(jnp.sum(folded, axis=1, keepdims=True) * FACTOR)
            spreads.append(spread.astype(BF16))
        for b in batch:
            suf_copies[b].wait()
        raw = [
            lax.dot_general(
                spread, suf[b, :, :KW], NT, preferred_element_type=F32
            )
            for b, spread in zip(batch, spreads)
        ]
        level = lse_all[...]
        for b, own_score, scores in zip(batch, own_scores, raw):
            scores = jnp.where(pos < slen_ref[0, b], scores * FACTOR, NEG)
            top = jnp.maximum(jnp.max(scores, axis=1, keepdims=True), own_score)
            weights = jnp.exp2(scores - top)
            own_weight = jnp.exp2(own_score - top)
            norm = jnp.sum(weights, axis=1, keepdims=True) + own_weight
            wide = jnp.dot(
                weights.astype(BF16), suf[b, :, KW:], preferred_element_type=F32
            )
            wide = wide + own_weight.astype(BF16).astype(F32) * new32[b : b + 1, KW:]
            result = jnp.where(row_group == 0, wide[:, :HD], 0.0)
            for g in range(1, KVH):
                result = jnp.where(
                    row_group == g, wide[:, g * HD : (g + 1) * HD], result
                )
            orow[pl.ds(b, H, stride=count), :] = result / norm
            level = jnp.where(lane == b, top + jnp.log2(norm), level)
        lse_all[...] = level

    for c, upto in enumerate(EARLY):

        @pl.when(chip == c)
        def _():
            for b in range(0, upto, 2):
                suffix(b)


    pl.semaphore_wait(barrier, n - 1)
    def q_copy(k, d):
        to = (me + d) % n
        col = (to % 2) * HALF_W + k * GW
        return remote(
            q_ref.at[:, pl.ds(pl.multiple_of(col, GW), GW)],
            qall.at[k, me],
            q_send.at[k],
            q_recv.at[k],
            to,
        )

    def q_wait(k):
        block = qall.at[k, pl.ds(0, n - 1)]
        return remote(block, block, q_send.at[k], q_recv.at[k], partner)

    order = sorted(range(1, n), key=lambda d: -min(d, n - d))
    for k in range(HALF_G):
        for d in order:
            q_copy(k, d).start()
    for part in range(2):
        kv_remote(0, part).start()
    for k in range(HALF_G):
        left = q_ref[:, k * GW : (k + 1) * GW]
        right = q_ref[:, HALF_W + k * GW : HALF_W + (k + 1) * GW]
        qall[k, me] = jnp.where(core == 0, left, right)

    for b in range(0, count, 2):
        skip = sum(upto > b for upto in EARLY)
        if skip:

            @pl.when(chip >= skip)
            def _():
                suffix(b)

        else:
            suffix(b)
        if b == count - 4:
            for part in range(2):
                kv_remote(1, part).start()

    for h in range(H):
        half, col = h // HALF_H, (h % HALF_H) * HD
        ssrc[half, :, col : col + HD] = orow[h * count : (h + 1) * count, :].astype(BF16)
    for half in range(2):
        lse_src[half] = lse_all[half * HALF_H : (half + 1) * HALF_H, :]
    s_copy = remote(ssrc.at[1 - core], sother, s_send.at[0], s_recv.at[0], partner)
    t_copy = remote(lse_src.at[1 - core], lse_other, s_send.at[1], s_recv.at[1], partner)
    t_copy.start()
    s_copy.start()
    for k in range(2, HALF_G):
        for part in range(2):
            kv_remote(k, part).start()
    owner_in.wait()
    plen_in.wait()
    owner = owner_ref[0]
    owner_chip = owner // 2
    slot = owner % 2
    plen = plen_ref[0]
    positions = kv0.shape[2]
    bias = jnp.where(
        lax.broadcasted_iota(jnp.int32, (1, positions), 1) < plen, 0.0, NEG
    ).astype(F32)
    wide_lane = lax.broadcasted_iota(jnp.int32, (total, HD), 1)

    def join_suffix():
        t_copy.wait_recv()
        lse_suf[...] = lse_src[core] + lse_other[...]
        turned[...] = jnp.concatenate(
            [lse_suf[...], jnp.zeros((HD - HALF_H, span), F32)], axis=0
        ).T
        first = pl.multiple_of(total + chip * both, both)
        scol[...] = turned[pl.ds(first, both), :]
        s_copy.wait_recv()
        s_own = ssrc[core].astype(F32)
        s_new = sother[...].astype(F32)
        s16[:count, :] = jnp.where(core == 0, s_own, s_new)
        s16[count:, :] = jnp.where(core == 0, s_new, s_own)

    away = 1 - 2 * near
    near_count = chip * (1 - near) + (chips - 1 - chip) * near
    far_count = chips - 1 - near_count
    row_side = (
        lax.broadcasted_iota(jnp.int32, (total, HD), 0) // both - chip
    ) * away
    near_rows = row_side < 0
    own_rows = row_side == 0
    far_rows = row_side > 0
    owner_side = (owner_chip - chip) * away
    owner_near = owner_side < 0
    is_mine = owner_side == 0
    owner_far = owner_side > 0

    def lse_copy(k, d):
        return remote(
            lse.at[chip, k],
            lse.at[chip, k],
            lse_send.at[0],
            lse_recv.at[chip, k],
            (me + 2 * d) % n,
        )

    def lse_wait(k, c):
        block = lse.at[c, k]
        remote(block, block, lse_send.at[0], lse_recv.at[c, k], partner).wait_recv()

    def o_copy(way, s):
        first, size = PARCELS[s]
        part = pl.ds(first, size)
        return remote(
            leaving.at[way, part],
            arrived.at[way, part],
            o_send.at[way],
            o_recv.at[way, s],
            (me + n + 2 - 4 * way) % n,
        )

    def a_copy(s):
        first, size = PARCELS[s]
        part = pl.ds(first, size)
        return remote(attn.at[part], attn_in.at[part], a_send.at[0], a_recv.at[s], partner)

    def heads_of(s):
        first, size = PARCELS[s]
        return range(first, first + size)

    def suffix_rows(h):
        part = s16[:, h * HD : (h + 1) * HD]
        return jnp.concatenate([part] * chips, axis=0)

    def forward(way, h, here, came, weight, up_rows, down_rows, owner_up):
        x = jnp.where(is_mine, here, came)
        y = jnp.where(own_rows, suffix_rows(h), came)
        blend = y + weight * (x - y)
        mixed = (up_rows & is_mine) | (own_rows & (owner_up | is_mine))
        out = jnp.where(down_rows, x, jnp.where(mixed, blend, y))
        leaving[way, h] = out.astype(BF16)

    def head(k):
        kv_wait(k)
        q_wait(k).wait_recv()
        rows = [
            qall[k, :, :, j * HD : (j + 1) * HD].astype(F32).reshape(total, HD)
            for j in range(GROUP)
        ]
        query = jnp.concatenate(rows, axis=0).astype(BF16)
        scores = lax.dot_general(query, kv[k][slot, 0], NT, preferred_element_type=F32)
        scores = scores * FACTOR + bias
        keep = kv[k][slot, 1]
        stats = jnp.zeros((total, HD), F32)
        for part in range(2):
            size = GROUP // 2 * total
            piece = scores[part * size : (part + 1) * size]
            top = jnp.max(piece, axis=1, keepdims=True)
            weights = jnp.exp2(piece - top)
            norm = jnp.sum(weights, axis=1, keepdims=True)
            result = jnp.dot(weights.astype(BF16), keep, preferred_element_type=F32)
            result = (result / norm).astype(BF16)
            level = top + jnp.log2(norm)
            for j in range(GROUP // 2):
                h = k * GROUP + part * GROUP // 2 + j
                rows = slice(j * total, (j + 1) * total)
                mine[h] = result[rows]
                stats = jnp.where(wide_lane == h, level[rows], stats)
        rows = slice(k * GROUP, (k + 1) * GROUP)
        flat = jnp.concatenate([stats, jnp.zeros((span - total, HD), F32)], axis=0).T
        if k == 0:
            join_suffix()
        lse[chip, k] = flat[rows, :] + lse_suf[rows, :]
        for d in range(1, chips):
            lse_copy(k, d).start()
        depart(parcels(k), stats)
    def parcels(k):
        return [s for s, (first, _) in enumerate(PARCELS) if first // GROUP == k]

    def depart(group, stats):
        @pl.when(at_end)
        def _():
            level = jnp.concatenate([scol[...]] * chips, axis=0)
            local = 1.0 / (1.0 + jnp.exp2(level - stats))
            for s in group:
                for h in heads_of(s):
                    block = mine[h]
                    arrived[near, h] = block
                    here = block.astype(F32)
                    weight = jnp.broadcast_to(local[:, h : h + 1], (total, HD))
                    forward(near, h, here, here, weight, near_rows, far_rows, owner_near)
                o_copy(near, s).start()

    def place(into, k, joined, source):
        gap = pltpu.roll(joined, total, 1) - source
        padded[:GROUP, :] = 1.0 / (1.0 + jnp.exp2(gap))
        column = padded[...].T[:total]
        for j in range(GROUP):
            into[k * GROUP + j] = jnp.broadcast_to(column[:, j : j + 1], (total, HD))

    def near_shares(k):
        own = lse[chip, k]
        joined, source = own, own
        for step in range(1, chips // 2):
            c = (chip + chips - away * step) % chips

            @pl.when(near_count >= step)
            def _():
                lse_wait(k, c)

            block = lse[c, k]
            joined = joined + jnp.where(near_count >= step, block, 0.0)
            source = jnp.where(owner_side == -step, block, source)
        place(near_share, k, joined, source)

    def shares(k):
        for step in range(1, chips):

            @pl.when(far_count >= step)
            def _():
                lse_wait(k, (chip + chips + away * step) % chips)

        joined, source = lse[0, k], lse[0, k]
        for c in range(1, chips):
            block = lse[c, k]
            joined = joined + block
            source = jnp.where(owner_chip == c, block, source)
        place(share, k, joined, source)

    def relay(s):
        o_copy(near, s).wait_recv()
        for h in heads_of(s):
            here = mine[h].astype(F32)
            came = arrived[near, h].astype(F32)
            forward(near, h, here, came, near_share[h], near_rows, far_rows, owner_near)
        o_copy(near, s).start()

    def finish(s):
        o_copy(1 - near, s).wait_recv()
        @pl.when(inside)
        def _():
            for h in heads_of(s):
                here = mine[h].astype(F32)
                far = arrived[1 - near, h].astype(F32)
                forward(1 - near, h, here, far, share[h], far_rows, near_rows, owner_far)
            o_copy(1 - near, s).start()

        for h in heads_of(s):
            here = mine[h].astype(F32)
            far = arrived[1 - near, h].astype(F32)
            close = arrived[near, h].astype(F32)
            x = jnp.where(is_mine, here, jnp.where(owner_near, close, far))
            y = jnp.where(own_rows, suffix_rows(h), jnp.where(near_rows, close, far))
            done = (near_rows & owner_near) | (far_rows & owner_far)
            attn[h] = jnp.where(done, y, y + share[h] * (x - y)).astype(BF16)
        a_copy(s).start()

    def project(block, half, pair):
        left = jnp.concatenate([block[2 * pair], block[2 * pair + 1]], axis=1)
        rows = wbuf[half, pair * 2 * HD : (pair + 1) * 2 * HD, :]
        return jnp.dot(left, rows, preferred_element_type=F32)

    def ready(pair, s):
        first, size = PARCELS[s]
        return first <= 2 * pair + 1 < first + size

    def inner(group, k):
        @pl.when(inside)
        def _():
            for s in group:
                if s == parcels(k)[0]:
                    near_shares(k)
                relay(s)

    for k in range(HALF_G):
        head(k)
        if k >= 2:
            inner(parcels(k - 2), k - 2)

    last = len(PARCELS)
    rest = [(s, k) for k in range(2, HALF_G) for s in parcels(k)]
    acc[...] = jnp.zeros(acc.shape, F32)
    pltpu.make_async_copy(wbuf, wbuf, w_sem.at[0]).wait()
    for s in range(last):
        k = PARCELS[s][0] // GROUP
        if rest:
            inner([rest[0][0]], rest[0][1])
            rest = rest[1:]
        if s == parcels(k)[0]:
            shares(k)
        finish(s)
        if s >= 1:
            for pair in range(PAIRS):
                if ready(pair, s - 1):
                    acc[...] = acc[...] + project(attn, core, pair)
        if s >= 3:
            a_copy(s - 3).wait_recv()
            for pair in range(PAIRS):
                if ready(pair, s - 3):
                    acc[...] = acc[...] + project(attn_in, 1 - core, pair)

    total_sum = acc[...]
    for pair in range(PAIRS):
        if ready(pair, last - 1):
            total_sum = total_sum + project(attn, core, pair)
    for s in range(last - 3, last):
        a_copy(s).wait_recv()
        for pair in range(PAIRS):
            if ready(pair, s):
                total_sum = total_sum + project(attn_in, 1 - core, pair)
    out_ref[0] = total_sum.astype(BF16)

    s_copy.wait_send()
    t_copy.wait_send()
    for k in range(HALF_G):
        q_wait(k).wait_send()
        sent = kv[k].at[core]
        remote(sent, sent, kv_send.at[k], kv_recv.at[k], partner).wait_send()
    remote(attn, attn, a_send.at[0], a_recv.at[0], partner).wait_send()
    block = lse.at[pl.ds(0, chips - 1)]
    remote(block, block, lse_send.at[0], lse_recv.at[0, 0], partner).wait_send()

    def sent_all(way):
        block = leaving.at[way]
        remote(block, block, o_send.at[way], o_recv.at[way, 0], partner).wait_send()

    sent_all(near)

    @pl.when(inside)
    def _():
        sent_all(1 - near)
def local(n, queries, prompt_cache, owner, prompt_len, suffix_cache, suffix_len, new_kv, out_weight):
    count = queries.shape[1]
    total = n * count
    chips = n // 2
    span = 2 * total
    slen = suffix_cache.shape[2]
    positions = prompt_cache.shape[2]
    width = out_weight.shape[1]
    hbm = pl.BlockSpec(memory_space=pltpu.HBM)
    vmem = pltpu.VMEM
    smem = pltpu.SMEM
    dma = pltpu.SemaphoreType.DMA
    stream = vmem((2, HALF_H, total, HD), BF16)
    chunk = vmem((HALF_H, total, HD), BF16)
    last = len(PARCELS)
    return pl.pallas_call(
        functools.partial(kernel, n),
        out_shape=pltpu.VMEM((1, total, width), BF16),
        in_specs=[hbm] * 8,
        out_specs=pl.BlockSpec(memory_space=pltpu.VMEM),
        scratch_shapes=[
            *[vmem((2, 2, positions, HD), BF16)] * HALF_G,
            vmem((count, slen, 2 * KW), BF16),
            vmem((2, HALF_W, width), BF16),
            smem((1,), jnp.int32),
            smem((1,), jnp.int32),
            smem((1, count), jnp.int32),
            vmem((count, H * HD), BF16),
            vmem((count, 2 * KW), BF16),
            vmem((HALF_G, n, count, GW), BF16),
            vmem((H * count, HD), F32),
            vmem((H * count, HD), F32),
            vmem((2, count, HALF_W), BF16),
            vmem((count, HALF_W), BF16),
            vmem((2 * count, HALF_W), F32),
            vmem((H, span), F32),
            vmem((2, HALF_H, span), F32),
            vmem((HALF_H, span), F32),
            vmem((HALF_H, span), F32),
            vmem((span, HD), F32),
            vmem((2 * count, HD), F32),
            vmem((chips, HALF_G, GROUP, span), F32),
            vmem((HD, span), F32),
            vmem((HALF_H, total, HD), F32),
            vmem((HALF_H, total, HD), F32),
            chunk,
            stream,
            stream,
            chunk,
            chunk,
            vmem((total, width), F32),
            dma((5,)),
            dma((count,)),
            dma((HALF_G,)),
            dma((1,)),
            dma((HALF_G,)),
            dma((HALF_G,)),
            dma((2,)),
            dma((2,)),
            dma((HALF_G,)),
            dma((HALF_G,)),
            dma((1,)),
            dma((chips, HALF_G)),
            dma((2,)),
            dma((2, last)),
            dma((1,)),
            dma((last,)),
        ],
        compiler_params=pltpu.CompilerParams(
            collective_id=0, has_side_effects=True, vmem_limit_bytes=60 * 1024 * 1024
        ),
        name="shared_decode",
    )(owner, prompt_len, suffix_len, queries, new_kv, prompt_cache, suffix_cache, out_weight)


def solution(mesh):
    in_specs = (
        P("prompt", "sample", None),
        P("prompt", "sample", None, None),
        P("prompt"),
        P("prompt"),
        P("prompt", "sample", None, None),
        P("prompt", "sample"),
        P("prompt", "sample", None),
        P(None, "sample"),
    )
    out_specs = P("prompt", None, "sample")
    body = functools.partial(local, mesh.shape["sample"])
    return jax.shard_map(body, mesh=mesh, in_specs=in_specs, out_specs=out_specs, check_vma=False)
```

```python
import functools

import jax
import jax.numpy as jnp
from jax import lax
from jax.experimental import pallas as pl
from jax.experimental.pallas import tpu as pltpu
from jax.sharding import PartitionSpec as P

H = 32
KVH = 8
HD = 128
GROUP = H // KVH
HALF_H = H // 2
HALF_G = KVH // 2
HALF_W = HALF_H * HD
KW = KVH * HD
GW = GROUP * HD
PAIRS = HALF_H // 2
PARCELS = ((0, 2), (2, 2), (4, 2), (6, 2), (8, 2), (10, 2), (12, 2), (14, 1), (15, 1))
EARLY = (4, 2)
LAG = 0
BEHIND = 2
BATCHES = {3: ((0, 3), (0, 2)), 5: ((3, 5), (2, 4))}
EDGES = (2, 4, 7)
FACTOR = HD ** (-0.5) * 1.4426950408889634
NEG = -1e30
F32 = jnp.float32
BF16 = jnp.bfloat16
NT = (((1,), (1,)), ((), ()))


def kernel(
    n,
    owner_hbm,
    plen_hbm,
    slen_hbm,
    q_hbm,
    new_hbm,
    cache_ref,
    suffix_ref,
    w_ref,
    out_ref,
    kv0,
    kv1,
    kv2,
    kv3,
    suf,
    wbuf,
    owner_ref,
    plen_ref,
    slen_ref,
    q_ref,
    new_ref,
    qall,
    qrow,
    orow,
    ssrc,
    sother,
    s16,
    lse_all,
    lse_src,
    lse_other,
    lse_suf,
    turned,
    scol,
    lse,
    padded,
    share,
    near_share,
    mine,
    arrived,
    leaving,
    attn,
    attn_in,
    acc,
    in_sem,
    suf_sem,
    kv_sem,
    w_sem,
    q_send,
    q_recv,
    s_send,
    s_recv,
    kv_send,
    kv_recv,
    lse_send,
    lse_recv,
    o_send,
    o_recv,
    a_send,
    a_recv,
):
    kv = (kv0, kv1, kv2, kv3)
    me = lax.axis_index("sample")
    chip = me // 2
    core = me % 2
    chips = n // 2
    partner = chip * 2 + (1 - core)
    count = q_ref.shape[0]
    total = n * count
    both = 2 * count
    span = 2 * total
    slen = suffix_ref.shape[2]
    near = chip // (chips // 2)
    away = 1 - 2 * near
    at_end = (chip == 0) | (chip == chips - 1)
    inside = (chip > 0) & (chip < chips - 1)

    def remote(src, dst, send, recv, to):
        return pltpu.make_async_remote_copy(
            src_ref=src,
            dst_ref=dst,
            send_sem=send,
            recv_sem=recv,
            device_id={"sample": to},
            device_id_type=pl.DeviceIdType.MESH,
        )

    barrier = pltpu.get_barrier_semaphore()
    for d in range(1, n):
        pl.semaphore_signal(
            barrier,
            inc=1,
            device_id={"sample": (me + d) % n},
            device_id_type=pl.DeviceIdType.MESH,
        )

    q_in = pltpu.make_async_copy(q_hbm.at[0], q_ref, in_sem.at[0])
    new_in = pltpu.make_async_copy(new_hbm.at[0], new_ref, in_sem.at[1])
    slen_in = pltpu.make_async_copy(slen_hbm, slen_ref, in_sem.at[2])
    owner_in = pltpu.make_async_copy(owner_hbm, owner_ref, in_sem.at[3])
    plen_in = pltpu.make_async_copy(plen_hbm, plen_ref, in_sem.at[4])
    suf_copies = [
        pltpu.make_async_copy(suffix_ref.at[0, b], suf.at[b], suf_sem.at[b // 2])
        for b in range(count)
    ]
    q_in.start()
    slen_in.start()
    new_in.start()
    for copy in suf_copies[:2]:
        copy.start()

    def kv_local(k, part):
        col = part * KW + (core * HALF_G + k) * HD
        return pltpu.make_async_copy(
            cache_ref.at[0, 0, :, pl.ds(pl.multiple_of(col, HD), HD)],
            kv[k].at[core, part],
            kv_sem.at[k],
        )

    def kv_remote(k, part):
        col = part * KW + ((1 - core) * HALF_G + k) * HD
        return remote(
            cache_ref.at[0, 0, :, pl.ds(pl.multiple_of(col, HD), HD)],
            kv[k].at[core, part],
            kv_send.at[k],
            kv_recv.at[k],
            partner,
        )

    def kv_wait(k):
        here = kv[k].at[core]
        pltpu.make_async_copy(here, here, kv_sem.at[k]).wait()
        there = kv[k].at[1 - core]
        remote(there, there, kv_send.at[k], kv_recv.at[k], partner).wait_recv()

    def w_copy(half):
        return pltpu.make_async_copy(
            w_ref.at[pl.ds(half * HALF_W, HALF_W), :], wbuf.at[half], w_sem.at[0]
        )

    padded[...] = jnp.zeros(padded.shape, F32)
    lse_all[...] = jnp.zeros(lse_all.shape, F32)
    q_in.wait()
    for copy in suf_copies[2:]:
        copy.start()
    q32 = q_ref[...].astype(F32)
    for h in range(H):
        qrow[h * count : (h + 1) * count, :] = q32[:, h * HD : (h + 1) * HD]
    new_in.wait()
    slen_in.wait()
    owner_in.start()
    plen_in.start()
    for k in range(HALF_G):
        for part in range(2):
            kv_local(k, part).start()
    for half in range(2):
        w_copy(half).start()
    new32 = new_ref[...].astype(F32)

    row_group = lax.broadcasted_iota(jnp.int32, (H, HD), 0) // GROUP
    lane = lax.broadcasted_iota(jnp.int32, (H, span), 1) - (total + me * count)
    pos = lax.broadcasted_iota(jnp.int32, (1, slen), 1)

    def suffix(first):
        batch = range(first, first + 2)
        spreads, own_scores = [], []
        for b in batch:
            query = qrow[pl.ds(b, H, stride=count), :]
            spread = jnp.concatenate(
                [jnp.where(row_group == g, query, 0.0) for g in range(KVH)], axis=1
            )
            own = spread * new32[b : b + 1, :KW]
            folded = own[:, :HD]
            for g in range(1, KVH):
                folded = folded + own[:, g * HD : (g + 1) * HD]
            own_scores.append(jnp.sum(folded, axis=1, keepdims=True) * FACTOR)
            spreads.append(spread.astype(BF16))
        block = suf.at[pl.ds(first, 2)]
        pltpu.make_async_copy(block, block, suf_sem.at[first // 2]).wait()
        raw = [
            lax.dot_general(
                spread, suf[b, :, :KW], NT, preferred_element_type=F32
            )
            for b, spread in zip(batch, spreads)
        ]
        level = lse_all[...]
        for b, own_score, scores in zip(batch, own_scores, raw):
            scores = jnp.where(pos < slen_ref[0, b], scores * FACTOR, NEG)
            top = jnp.maximum(jnp.max(scores, axis=1, keepdims=True), own_score)
            weights = jnp.exp2(scores - top)
            own_weight = jnp.exp2(own_score - top)
            norm = jnp.sum(weights, axis=1, keepdims=True) + own_weight
            wide = jnp.dot(
                weights.astype(BF16), suf[b, :, KW:], preferred_element_type=F32
            )
            wide = wide + own_weight.astype(BF16).astype(F32) * new32[b : b + 1, KW:]
            result = jnp.where(row_group == 0, wide[:, :HD], 0.0)
            for g in range(1, KVH):
                result = jnp.where(
                    row_group == g, wide[:, g * HD : (g + 1) * HD], result
                )
            orow[pl.ds(b, H, stride=count), :] = result / norm
            level = jnp.where(lane == b, top + jnp.log2(norm), level)
        lse_all[...] = level

    for c, upto in enumerate(EARLY):

        @pl.when(chip == c)
        def _():
            for b in range(0, upto, 2):
                suffix(b)


    pl.semaphore_wait(barrier, n - 1)
    def q_copy(k, to):
        col = (to % 2) * HALF_W + k * GW
        return remote(
            q_ref.at[:, pl.ds(pl.multiple_of(col, GW), GW)],
            qall.at[k, me],
            q_send.at[0],
            q_recv.at[k],
            to,
        )

    def q_wait(k):
        block = qall.at[k, pl.ds(0, n - 1)]
        return remote(block, block, q_send.at[0], q_recv.at[k], partner)

    amid = jnp.where(inside, 1, 0)
    reach = list(range(chips - 1, 0, -1))
    if len(reach) > 1:
        reach[0], reach[1] = chips - 1 - amid, chips - 2 + amid
    sends = sorted(
        (k + LAG * (rank >= 2), rank, k)
        for rank in range(len(reach))
        for k in range(HALF_G)
    )
    for _, rank, k in sends:
        for other in range(2):
            q_copy(k, (chip + chips + away * reach[rank]) % chips * 2 + other).start()
    for k in range(HALF_G):
        q_copy(k, partner).start()
    for part in range(2):
        kv_remote(0, part).start()
    for k in range(HALF_G):
        left = q_ref[:, k * GW : (k + 1) * GW]
        right = q_ref[:, HALF_W + k * GW : HALF_W + (k + 1) * GW]
        qall[k, me] = jnp.where(core == 0, left, right)

    for b in range(0, count, 2):
        skip = sum(upto > b for upto in EARLY)
        if skip:

            @pl.when(chip >= skip)
            def _():
                suffix(b)

        else:
            suffix(b)
        if b == count - 4:
            for part in range(2):
                kv_remote(1, part).start()

    for h in range(H):
        half, col = h // HALF_H, (h % HALF_H) * HD
        ssrc[half, :, col : col + HD] = orow[h * count : (h + 1) * count, :].astype(BF16)
    for half in range(2):
        lse_src[half] = lse_all[half * HALF_H : (half + 1) * HALF_H, :]
    s_copy = remote(ssrc.at[1 - core], sother, s_send.at[0], s_recv.at[0], partner)
    t_copy = remote(lse_src.at[1 - core], lse_other, s_send.at[1], s_recv.at[1], partner)
    t_copy.start()
    s_copy.start()
    for k in range(2, HALF_G):
        for part in range(2):
            kv_remote(k, part).start()
    owner_in.wait()
    plen_in.wait()
    owner = owner_ref[0]
    owner_chip = owner // 2
    slot = owner % 2
    plen = plen_ref[0]
    positions = kv0.shape[2]
    bias = jnp.where(
        lax.broadcasted_iota(jnp.int32, (1, positions), 1) < plen, 0.0, NEG
    ).astype(F32)
    wide_lane = lax.broadcasted_iota(jnp.int32, (total, HD), 1)

    def join_suffix():
        t_copy.wait_recv()
        lse_suf[...] = lse_src[core] + lse_other[...]
        turned[...] = jnp.concatenate(
            [lse_suf[...], jnp.zeros((HD - HALF_H, span), F32)], axis=0
        ).T
        first = pl.multiple_of(total + chip * both, both)
        scol[...] = turned[pl.ds(first, both), :]
        s_copy.wait_recv()
        s_own = ssrc[core].astype(F32)
        s_new = sother[...].astype(F32)
        s16[:count, :] = jnp.where(core == 0, s_own, s_new)
        s16[count:, :] = jnp.where(core == 0, s_new, s_own)

    near_count = chip * (1 - near) + (chips - 1 - chip) * near
    far_count = chips - 1 - near_count
    row_side = (
        lax.broadcasted_iota(jnp.int32, (total, HD), 0) // both - chip
    ) * away
    near_rows = row_side < 0
    own_rows = row_side == 0
    far_rows = row_side > 0
    owner_side = (owner_chip - chip) * away
    owner_near = owner_side < 0
    is_mine = owner_side == 0
    owner_far = owner_side > 0

    def lse_copy(k, d):
        to = (chip + d) % chips
        side = 1 - 2 * (to // (chips // 2))
        far = jnp.where((chip - to) * side > 0, 1, 0)
        return remote(
            lse.at[chip, k],
            lse.at[chip, k],
            lse_send.at[0],
            lse_recv.at[far, k],
            (me + 2 * d) % n,
        )

    def lse_wait(k, far, messages):
        block = lse.at[pl.ds(0, messages), k]
        remote(block, block, lse_send.at[0], lse_recv.at[far, k], partner).wait_recv()

    def o_copy(way, s):
        first, size = PARCELS[s]
        part = pl.ds(first, size)
        return remote(
            leaving.at[way, part],
            arrived.at[way, part],
            o_send.at[way],
            o_recv.at[way, s],
            (me + n + 2 - 4 * way) % n,
        )

    def a_copy(s):
        first, size = PARCELS[s]
        part = pl.ds(first, size)
        return remote(attn.at[part], attn_in.at[part], a_send.at[0], a_recv.at[batch_of(s)], partner)

    def batch_of(s):
        return sum(PARCELS[s][0] >= 2 * edge for edge in EDGES)

    def heads_of(s):
        first, size = PARCELS[s]
        return range(first, first + size)

    def suffix_rows(h):
        part = s16[:, h * HD : (h + 1) * HD]
        return jnp.concatenate([part] * chips, axis=0)

    def forward(way, h, here, came, weight, up_rows, down_rows, owner_up):
        x = jnp.where(is_mine, here, came)
        y = jnp.where(own_rows, suffix_rows(h), came)
        blend = y + weight * (x - y)
        mixed = (up_rows & is_mine) | (own_rows & (owner_up | is_mine))
        out = jnp.where(down_rows, x, jnp.where(mixed, blend, y))
        leaving[way, h] = out.astype(BF16)

    def head(k):
        kv_wait(k)
        q_wait(k).wait_recv()
        rows = [
            qall[k, :, :, j * HD : (j + 1) * HD].astype(F32).reshape(total, HD)
            for j in range(GROUP)
        ]
        query = jnp.concatenate(rows, axis=0).astype(BF16)
        scores = lax.dot_general(query, kv[k][slot, 0], NT, preferred_element_type=F32)
        scores = scores * FACTOR + bias
        keep = kv[k][slot, 1]
        stats = jnp.zeros((total, HD), F32)
        for part in range(2):
            size = GROUP // 2 * total
            piece = scores[part * size : (part + 1) * size]
            top = jnp.max(piece, axis=1, keepdims=True)
            weights = jnp.exp2(piece - top)
            norm = jnp.sum(weights, axis=1, keepdims=True)
            result = jnp.dot(weights.astype(BF16), keep, preferred_element_type=F32)
            result = (result / norm).astype(BF16)
            level = top + jnp.log2(norm)
            for j in range(GROUP // 2):
                h = k * GROUP + part * GROUP // 2 + j
                rows = slice(j * total, (j + 1) * total)
                mine[h] = result[rows]
                stats = jnp.where(wide_lane == h, level[rows], stats)
        rows = slice(k * GROUP, (k + 1) * GROUP)
        flat = jnp.concatenate([stats, jnp.zeros((span - total, HD), F32)], axis=0).T
        if k == 0:
            join_suffix()
        lse[chip, k] = flat[rows, :] + lse_suf[rows, :]
        for d in range(1, chips):
            lse_copy(k, d).start()
        depart(parcels(k), stats)
    def parcels(k):
        return [s for s, (first, _) in enumerate(PARCELS) if first // GROUP == k]

    def depart(group, stats):
        @pl.when(at_end)
        def _():
            level = jnp.concatenate([scol[...]] * chips, axis=0)
            local = 1.0 / (1.0 + jnp.exp2(level - stats))
            for s in group:
                for h in heads_of(s):
                    block = mine[h]
                    arrived[near, h] = block
                    here = block.astype(F32)
                    weight = jnp.broadcast_to(local[:, h : h + 1], (total, HD))
                    forward(near, h, here, here, weight, near_rows, far_rows, owner_near)
                o_copy(near, s).start()

    def place(into, k, joined, source):
        padded[0, :GROUP, :] = joined
        padded[1, :GROUP, :] = source
        gap = padded[0].T[total:] - padded[1].T[:total]
        column = 1.0 / (1.0 + jnp.exp2(gap))
        for j in range(GROUP):
            into[k * GROUP + j] = jnp.broadcast_to(column[:, j : j + 1], (total, HD))

    def near_shares(k):
        for step in range(1, chips // 2):

            @pl.when(near_count == step)
            def _():
                lse_wait(k, 0, step)

        own = lse[chip, k]
        joined, source = own, own
        for step in range(1, chips // 2):
            c = (chip + chips - away * step) % chips
            block = lse[c, k]
            joined = joined + jnp.where(near_count >= step, block, 0.0)
            source = jnp.where(owner_side == -step, block, source)
        place(near_share, k, joined, source)

    def shares(k):
        for step in range(chips // 2, chips):

            @pl.when(far_count == step)
            def _():
                lse_wait(k, 1, step)

        joined, source = lse[0, k], lse[0, k]
        for c in range(1, chips):
            block = lse[c, k]
            joined = joined + block
            source = jnp.where(owner_chip == c, block, source)
        place(share, k, joined, source)

    def relay(s):
        o_copy(near, s).wait_recv()
        for h in heads_of(s):
            here = mine[h].astype(F32)
            came = arrived[near, h].astype(F32)
            forward(near, h, here, came, near_share[h], near_rows, far_rows, owner_near)
        o_copy(near, s).start()

    def finish(s):
        o_copy(1 - near, s).wait_recv()
        @pl.when(inside)
        def _():
            for h in heads_of(s):
                here = mine[h].astype(F32)
                far = arrived[1 - near, h].astype(F32)
                forward(1 - near, h, here, far, share[h], far_rows, near_rows, owner_far)
            o_copy(1 - near, s).start()

        for h in heads_of(s):
            here = mine[h].astype(F32)
            far = arrived[1 - near, h].astype(F32)
            close = arrived[near, h].astype(F32)
            x = jnp.where(is_mine, here, jnp.where(owner_near, close, far))
            y = jnp.where(own_rows, suffix_rows(h), jnp.where(near_rows, close, far))
            done = (near_rows & owner_near) | (far_rows & owner_far)
            attn[h] = jnp.where(done, y, y + share[h] * (x - y)).astype(BF16)
        a_copy(s).start()

    def project(block, half, pair):
        left = jnp.concatenate([block[2 * pair], block[2 * pair + 1]], axis=1)
        rows = wbuf[half, pair * 2 * HD : (pair + 1) * 2 * HD, :]
        return jnp.dot(left, rows, preferred_element_type=F32)

    def ready(pair, s):
        first, size = PARCELS[s]
        return first <= 2 * pair + 1 < first + size

    def inner(group, k):
        @pl.when(inside)
        def _():
            for s in group:
                if s == parcels(k)[0]:
                    near_shares(k)
                relay(s)

    for k in range(HALF_G):
        head(k)
        if k >= BEHIND:
            inner(parcels(k - BEHIND), k - BEHIND)

    last = len(PARCELS)
    rest = [(s, k) for k in range(HALF_G - BEHIND, HALF_G) for s in parcels(k)]
    pltpu.make_async_copy(wbuf, wbuf, w_sem.at[0]).wait()

    @pl.when(at_end)
    def _():
        for k in range(HALF_G):
            shares(k)

    def gather(first, stop):
        bounds = (0, *EDGES, PAIRS)
        for batch in range(len(EDGES) + 1):
            if first <= bounds[batch] < stop:
                block = attn_in.at[pl.ds(2 * bounds[batch], 2 * (bounds[batch + 1] - bounds[batch]))]
                remote(block, block, a_send.at[0], a_recv.at[batch], partner).wait_recv()

    def product(block, half, first, stop):
        sums = project(block, half, first)
        for pair in range(first + 1, stop):
            sums = sums + project(block, half, pair)
        return sums

    for s in range(last):
        k = PARCELS[s][0] // GROUP
        if rest:
            inner([rest[0][0]], rest[0][1])
            rest = rest[1:]
        if s == parcels(k)[0]:

            @pl.when(inside)
            def _():
                shares(k)

        finish(s)
        if s in BATCHES:

            @pl.when(at_end)
            def _():
                (own_from, own_to), (other_from, other_to) = BATCHES[s]
                part = product(attn, core, own_from, own_to)
                gather(other_from, other_to)
                part = part + product(attn_in, 1 - core, other_from, other_to)
                acc[...] = part if s == min(BATCHES) else acc[...] + part

    (_, own_at), (_, other_at) = BATCHES[max(BATCHES)]

    @pl.when(inside)
    def _():
        part = product(attn, core, 0, own_at)
        gather(0, other_at)
        acc[...] = part + product(attn_in, 1 - core, 0, other_at)

    total_sum = acc[...] + product(attn, core, own_at, PAIRS)
    gather(other_at, PAIRS - 1)
    total_sum = total_sum + product(attn_in, 1 - core, other_at, PAIRS - 1)
    gather(PAIRS - 1, PAIRS)
    total_sum = total_sum + product(attn_in, 1 - core, PAIRS - 1, PAIRS)
    out_ref[0] = total_sum.astype(BF16)

    s_copy.wait_send()
    t_copy.wait_send()
    for k in range(HALF_G):
        sent = kv[k].at[core]
        remote(sent, sent, kv_send.at[k], kv_recv.at[k], partner).wait_send()
    block = qall.at[:, pl.ds(0, n - 1)]
    remote(block, block, q_send.at[0], q_recv.at[0], partner).wait_send()
    remote(attn, attn, a_send.at[0], a_recv.at[0], partner).wait_send()
    block = lse.at[pl.ds(0, chips - 1)]
    remote(block, block, lse_send.at[0], lse_recv.at[0, 0], partner).wait_send()

    def sent_all(way):
        block = leaving.at[way]
        remote(block, block, o_send.at[way], o_recv.at[way, 0], partner).wait_send()

    sent_all(near)

    @pl.when(inside)
    def _():
        sent_all(1 - near)
def local(n, queries, prompt_cache, owner, prompt_len, suffix_cache, suffix_len, new_kv, out_weight):
    count = queries.shape[1]
    total = n * count
    chips = n // 2
    span = 2 * total
    slen = suffix_cache.shape[2]
    positions = prompt_cache.shape[2]
    width = out_weight.shape[1]
    hbm = pl.BlockSpec(memory_space=pltpu.HBM)
    vmem = pltpu.VMEM
    smem = pltpu.SMEM
    dma = pltpu.SemaphoreType.DMA
    stream = vmem((2, HALF_H, total, HD), BF16)
    chunk = vmem((HALF_H, total, HD), BF16)
    last = len(PARCELS)
    return pl.pallas_call(
        functools.partial(kernel, n),
        out_shape=pltpu.VMEM((1, total, width), BF16),
        in_specs=[hbm] * 8,
        out_specs=pl.BlockSpec(memory_space=pltpu.VMEM),
        scratch_shapes=[
            *[vmem((2, 2, positions, HD), BF16)] * HALF_G,
            vmem((count, slen, 2 * KW), BF16),
            vmem((2, HALF_W, width), BF16),
            smem((1,), jnp.int32),
            smem((1,), jnp.int32),
            smem((1, count), jnp.int32),
            vmem((count, H * HD), BF16),
            vmem((count, 2 * KW), BF16),
            vmem((HALF_G, n, count, GW), BF16),
            vmem((H * count, HD), F32),
            vmem((H * count, HD), F32),
            vmem((2, count, HALF_W), BF16),
            vmem((count, HALF_W), BF16),
            vmem((2 * count, HALF_W), F32),
            vmem((H, span), F32),
            vmem((2, HALF_H, span), F32),
            vmem((HALF_H, span), F32),
            vmem((HALF_H, span), F32),
            vmem((span, HD), F32),
            vmem((2 * count, HD), F32),
            vmem((chips, HALF_G, GROUP, span), F32),
            vmem((2, HD, span), F32),
            vmem((HALF_H, total, HD), F32),
            vmem((HALF_H, total, HD), F32),
            chunk,
            stream,
            stream,
            chunk,
            chunk,
            vmem((total, width), F32),
            dma((5,)),
            dma((count // 2,)),
            dma((HALF_G,)),
            dma((1,)),
            dma((1,)),
            dma((HALF_G,)),
            dma((2,)),
            dma((2,)),
            dma((HALF_G,)),
            dma((HALF_G,)),
            dma((1,)),
            dma((2, HALF_G)),
            dma((2,)),
            dma((2, last)),
            dma((1,)),
            dma((len(EDGES) + 1,)),
        ],
        compiler_params=pltpu.CompilerParams(
            collective_id=0, has_side_effects=True, vmem_limit_bytes=60 * 1024 * 1024
        ),
        name="shared_decode",
    )(owner, prompt_len, suffix_len, queries, new_kv, prompt_cache, suffix_cache, out_weight)


def solution(mesh):
    in_specs = (
        P("prompt", "sample", None),
        P("prompt", "sample", None, None),
        P("prompt"),
        P("prompt"),
        P("prompt", "sample", None, None),
        P("prompt", "sample"),
        P("prompt", "sample", None),
        P(None, "sample"),
    )
    out_specs = P("prompt", None, "sample")
    body = functools.partial(local, mesh.shape["sample"])
    return jax.shard_map(body, mesh=mesh, in_specs=in_specs, out_specs=out_specs, check_vma=False)
```

```python
import functools

import jax
import jax.numpy as jnp
from jax import lax
from jax.experimental import pallas as pl
from jax.experimental.pallas import tpu as pltpu
from jax.sharding import PartitionSpec as P

H = 32
KVH = 8
HD = 128
GROUP = H // KVH
HALF_H = H // 2
HALF_G = KVH // 2
HALF_W = HALF_H * HD
KW = KVH * HD
GW = GROUP * HD
PAIRS = HALF_H // 2
PARCELS = ((0, 2), (2, 2), (4, 2), (6, 2), (8, 2), (10, 2), (12, 2), (14, 2))
EARLY = (4, 2)
LAG = 0
BEHIND = 2
BATCHES = {3: ((0, 3), (0, 2)), 5: ((3, 6), (2, 4))}
EDGES = (2, 4, 7)
FACTOR = HD ** (-0.5) * 1.4426950408889634
NEG = -1e30
F32 = jnp.float32
BF16 = jnp.bfloat16
NT = (((1,), (1,)), ((), ()))


def kernel(
    n,
    owner_hbm,
    plen_hbm,
    slen_hbm,
    q_hbm,
    new_hbm,
    cache_ref,
    suffix_ref,
    w_ref,
    out_ref,
    kv0,
    kv1,
    kv2,
    kv3,
    suf,
    wbuf,
    owner_ref,
    plen_ref,
    slen_ref,
    q_ref,
    new_ref,
    qall,
    qrow,
    orow,
    ssrc,
    sother,
    s16,
    lse_all,
    lse_src,
    lse_other,
    lse_suf,
    turned,
    scol,
    lse,
    padded,
    share,
    near_share,
    mine,
    arrived,
    leaving,
    attn,
    attn_in,
    acc,
    in_sem,
    suf_sem,
    kv_sem,
    w_sem,
    q_send,
    q_recv,
    s_send,
    s_recv,
    kv_send,
    kv_recv,
    lse_send,
    lse_recv,
    o_send,
    o_recv,
    a_send,
    a_recv,
):
    kv = (kv0, kv1, kv2, kv3)
    me = lax.axis_index("sample")
    chip = me // 2
    core = me % 2
    chips = n // 2
    partner = chip * 2 + (1 - core)
    count = q_ref.shape[0]
    total = n * count
    both = 2 * count
    span = 2 * total
    slen = suffix_ref.shape[2]
    near = chip // (chips // 2)
    away = 1 - 2 * near
    at_end = (chip == 0) | (chip == chips - 1)
    inside = (chip > 0) & (chip < chips - 1)

    def remote(src, dst, send, recv, to):
        return pltpu.make_async_remote_copy(
            src_ref=src,
            dst_ref=dst,
            send_sem=send,
            recv_sem=recv,
            device_id={"sample": to},
            device_id_type=pl.DeviceIdType.MESH,
        )

    barrier = pltpu.get_barrier_semaphore()
    for d in range(1, n):
        pl.semaphore_signal(
            barrier,
            inc=1,
            device_id={"sample": (me + d) % n},
            device_id_type=pl.DeviceIdType.MESH,
        )

    q_in = pltpu.make_async_copy(q_hbm.at[0], q_ref, in_sem.at[0])
    new_in = pltpu.make_async_copy(new_hbm.at[0], new_ref, in_sem.at[1])
    slen_in = pltpu.make_async_copy(slen_hbm, slen_ref, in_sem.at[2])
    owner_in = pltpu.make_async_copy(owner_hbm, owner_ref, in_sem.at[3])
    plen_in = pltpu.make_async_copy(plen_hbm, plen_ref, in_sem.at[4])
    suf_copies = [
        pltpu.make_async_copy(suffix_ref.at[0, b], suf.at[b], suf_sem.at[b // 2])
        for b in range(count)
    ]
    q_in.start()
    slen_in.start()
    new_in.start()
    for copy in suf_copies[:2]:
        copy.start()

    def kv_local(k, part):
        col = part * KW + (core * HALF_G + k) * HD
        return pltpu.make_async_copy(
            cache_ref.at[0, 0, :, pl.ds(pl.multiple_of(col, HD), HD)],
            kv[k].at[core, part],
            kv_sem.at[k],
        )

    def kv_remote(k, part):
        col = part * KW + ((1 - core) * HALF_G + k) * HD
        return remote(
            cache_ref.at[0, 0, :, pl.ds(pl.multiple_of(col, HD), HD)],
            kv[k].at[core, part],
            kv_send.at[k],
            kv_recv.at[k],
            partner,
        )

    def kv_wait(k):
        here = kv[k].at[core]
        pltpu.make_async_copy(here, here, kv_sem.at[k]).wait()
        there = kv[k].at[1 - core]
        remote(there, there, kv_send.at[k], kv_recv.at[k], partner).wait_recv()

    def w_copy(half):
        return pltpu.make_async_copy(
            w_ref.at[pl.ds(half * HALF_W, HALF_W), :], wbuf.at[half], w_sem.at[0]
        )

    padded[...] = jnp.zeros(padded.shape, F32)
    lse_all[...] = jnp.zeros(lse_all.shape, F32)
    q_in.wait()
    for copy in suf_copies[2:]:
        copy.start()
    q32 = q_ref[...].astype(F32)
    for h in range(H):
        qrow[h * count : (h + 1) * count, :] = q32[:, h * HD : (h + 1) * HD]
    new_in.wait()
    slen_in.wait()
    owner_in.start()
    plen_in.start()
    for k in range(HALF_G):
        for part in range(2):
            kv_local(k, part).start()
    for half in range(2):
        w_copy(half).start()
    new32 = new_ref[...].astype(F32)

    row_group = lax.broadcasted_iota(jnp.int32, (H, HD), 0) // GROUP
    lane = lax.broadcasted_iota(jnp.int32, (H, span), 1) - (total + me * count)
    pos = lax.broadcasted_iota(jnp.int32, (1, slen), 1)

    def suffix(first):
        batch = range(first, first + 2)
        spreads, own_scores = [], []
        for b in batch:
            query = qrow[pl.ds(b, H, stride=count), :]
            spread = jnp.concatenate(
                [jnp.where(row_group == g, query, 0.0) for g in range(KVH)], axis=1
            )
            own = spread * new32[b : b + 1, :KW]
            folded = own[:, :HD]
            for g in range(1, KVH):
                folded = folded + own[:, g * HD : (g + 1) * HD]
            own_scores.append(jnp.sum(folded, axis=1, keepdims=True) * FACTOR)
            spreads.append(spread.astype(BF16))
        block = suf.at[pl.ds(first, 2)]
        pltpu.make_async_copy(block, block, suf_sem.at[first // 2]).wait()
        raw = [
            lax.dot_general(
                spread, suf[b, :, :KW], NT, preferred_element_type=F32
            )
            for b, spread in zip(batch, spreads)
        ]
        level = lse_all[...]
        for b, own_score, scores in zip(batch, own_scores, raw):
            scores = jnp.where(pos < slen_ref[0, b], scores * FACTOR, NEG)
            top = jnp.maximum(jnp.max(scores, axis=1, keepdims=True), own_score)
            weights = jnp.exp2(scores - top)
            own_weight = jnp.exp2(own_score - top)
            norm = jnp.sum(weights, axis=1, keepdims=True) + own_weight
            wide = jnp.dot(
                weights.astype(BF16), suf[b, :, KW:], preferred_element_type=F32
            )
            wide = wide + own_weight.astype(BF16).astype(F32) * new32[b : b + 1, KW:]
            result = jnp.where(row_group == 0, wide[:, :HD], 0.0)
            for g in range(1, KVH):
                result = jnp.where(
                    row_group == g, wide[:, g * HD : (g + 1) * HD], result
                )
            orow[pl.ds(b, H, stride=count), :] = result / norm
            level = jnp.where(lane == b, top + jnp.log2(norm), level)
        lse_all[...] = level

    for c, upto in enumerate(EARLY):

        @pl.when(chip == c)
        def _():
            for b in range(0, upto, 2):
                suffix(b)


    pl.semaphore_wait(barrier, n - 1)
    def q_copy(k, to):
        col = (to % 2) * HALF_W + k * GW
        return remote(
            q_ref.at[:, pl.ds(pl.multiple_of(col, GW), GW)],
            qall.at[k, me],
            q_send.at[0],
            q_recv.at[k],
            to,
        )

    def q_wait(k):
        block = qall.at[k, pl.ds(0, n - 1)]
        return remote(block, block, q_send.at[0], q_recv.at[k], partner)

    amid = jnp.where(inside, 1, 0)
    reach = list(range(chips - 1, 0, -1))
    if len(reach) > 1:
        reach[0], reach[1] = chips - 1 - amid, chips - 2 + amid
    sends = sorted(
        (k + LAG * (rank >= 2), rank, k)
        for rank in range(len(reach))
        for k in range(HALF_G)
    )
    for _, rank, k in sends:
        for other in range(2):
            q_copy(k, (chip + chips + away * reach[rank]) % chips * 2 + other).start()
    for k in range(HALF_G):
        q_copy(k, partner).start()
    for part in range(2):
        kv_remote(0, part).start()
    for k in range(HALF_G):
        left = q_ref[:, k * GW : (k + 1) * GW]
        right = q_ref[:, HALF_W + k * GW : HALF_W + (k + 1) * GW]
        qall[k, me] = jnp.where(core == 0, left, right)

    for b in range(0, count, 2):
        skip = sum(upto > b for upto in EARLY)
        if skip:

            @pl.when(chip >= skip)
            def _():
                suffix(b)

        else:
            suffix(b)
        if b == count - 4:
            for part in range(2):
                kv_remote(1, part).start()

    for h in range(H):
        half, col = h // HALF_H, (h % HALF_H) * HD
        ssrc[half, :, col : col + HD] = orow[h * count : (h + 1) * count, :].astype(BF16)
    for half in range(2):
        lse_src[half] = lse_all[half * HALF_H : (half + 1) * HALF_H, :]
    s_copy = remote(ssrc.at[1 - core], sother, s_send.at[0], s_recv.at[0], partner)
    t_copy = remote(lse_src.at[1 - core], lse_other, s_send.at[1], s_recv.at[1], partner)
    t_copy.start()
    s_copy.start()
    for k in range(2, HALF_G):
        for part in range(2):
            kv_remote(k, part).start()
    owner_in.wait()
    plen_in.wait()
    owner = owner_ref[0]
    owner_chip = owner // 2
    slot = owner % 2
    plen = plen_ref[0]
    positions = kv0.shape[2]
    bias = jnp.where(
        lax.broadcasted_iota(jnp.int32, (1, positions), 1) < plen, 0.0, NEG
    ).astype(F32)
    wide_lane = lax.broadcasted_iota(jnp.int32, (total, HD), 1)

    def join_suffix():
        t_copy.wait_recv()
        lse_suf[...] = lse_src[core] + lse_other[...]
        turned[...] = jnp.concatenate(
            [lse_suf[...], jnp.zeros((HD - HALF_H, span), F32)], axis=0
        ).T
        first = pl.multiple_of(total + chip * both, both)
        scol[...] = turned[pl.ds(first, both), :]
        s_copy.wait_recv()
        s_own = ssrc[core].astype(F32)
        s_new = sother[...].astype(F32)
        s16[:count, :] = jnp.where(core == 0, s_own, s_new)
        s16[count:, :] = jnp.where(core == 0, s_new, s_own)

    near_count = chip * (1 - near) + (chips - 1 - chip) * near
    far_count = chips - 1 - near_count
    row_side = (
        lax.broadcasted_iota(jnp.int32, (total, HD), 0) // both - chip
    ) * away
    near_rows = row_side < 0
    own_rows = row_side == 0
    far_rows = row_side > 0
    owner_side = (owner_chip - chip) * away
    owner_near = owner_side < 0
    is_mine = owner_side == 0
    owner_far = owner_side > 0

    def lse_copy(k, d):
        to = (chip + d) % chips
        side = 1 - 2 * (to // (chips // 2))
        far = jnp.where((chip - to) * side > 0, 1, 0)
        return remote(
            lse.at[chip, k],
            lse.at[chip, k],
            lse_send.at[0],
            lse_recv.at[far, k],
            (me + 2 * d) % n,
        )

    def lse_wait(k, far, messages):
        block = lse.at[pl.ds(0, messages), k]
        remote(block, block, lse_send.at[0], lse_recv.at[far, k], partner).wait_recv()

    def o_copy(way, s):
        first, size = PARCELS[s]
        part = pl.ds(first, size)
        return remote(
            leaving.at[way, part],
            arrived.at[way, part],
            o_send.at[way],
            o_recv.at[way, s],
            (me + n + 2 - 4 * way) % n,
        )

    def a_copy(s):
        first, size = PARCELS[s]
        part = pl.ds(first, size)
        return remote(attn.at[part], attn_in.at[part], a_send.at[0], a_recv.at[batch_of(s)], partner)

    def batch_of(s):
        return sum(PARCELS[s][0] >= 2 * edge for edge in EDGES)

    def heads_of(s):
        first, size = PARCELS[s]
        return range(first, first + size)

    def suffix_rows(h):
        part = s16[:, h * HD : (h + 1) * HD]
        return jnp.concatenate([part] * chips, axis=0)

    def forward(way, h, here, came, weight, up_rows, down_rows, owner_up):
        x = jnp.where(is_mine, here, came)
        y = jnp.where(own_rows, suffix_rows(h), came)
        blend = y + weight * (x - y)
        mixed = (up_rows & is_mine) | (own_rows & (owner_up | is_mine))
        out = jnp.where(down_rows, x, jnp.where(mixed, blend, y))
        leaving[way, h] = out.astype(BF16)

    def head(k):
        kv_wait(k)
        q_wait(k).wait_recv()
        rows = [
            qall[k, :, :, j * HD : (j + 1) * HD].astype(F32).reshape(total, HD)
            for j in range(GROUP)
        ]
        query = jnp.concatenate(rows, axis=0).astype(BF16)
        scores = lax.dot_general(query, kv[k][slot, 0], NT, preferred_element_type=F32)
        scores = scores * FACTOR + bias
        keep = kv[k][slot, 1]
        stats = jnp.zeros((total, HD), F32)
        for part in range(1):
            size = GROUP * total
            piece = scores[part * size : (part + 1) * size]
            top = jnp.max(piece, axis=1, keepdims=True)
            weights = jnp.exp2(piece - top)
            norm = jnp.sum(weights, axis=1, keepdims=True)
            result = jnp.dot(weights.astype(BF16), keep, preferred_element_type=F32)
            result = (result / norm).astype(BF16)
            level = top + jnp.log2(norm)
            for j in range(GROUP):
                h = k * GROUP + j
                rows = slice(j * total, (j + 1) * total)
                mine[h] = result[rows]
                stats = jnp.where(wide_lane == h, level[rows], stats)
        rows = slice(k * GROUP, (k + 1) * GROUP)
        flat = jnp.concatenate([stats, jnp.zeros((span - total, HD), F32)], axis=0).T
        if k == 0:
            join_suffix()
        lse[chip, k] = flat[rows, :] + lse_suf[rows, :]
        for d in range(1, chips):
            lse_copy(k, d).start()
        depart(parcels(k), stats)
    def parcels(k):
        return [s for s, (first, _) in enumerate(PARCELS) if first // GROUP == k]

    def depart(group, stats):
        @pl.when(at_end)
        def _():
            level = jnp.concatenate([scol[...]] * chips, axis=0)
            local = 1.0 / (1.0 + jnp.exp2(level - stats))
            for s in group:
                for h in heads_of(s):
                    block = mine[h]
                    arrived[near, h] = block
                    here = block.astype(F32)
                    weight = jnp.broadcast_to(local[:, h : h + 1], (total, HD))
                    forward(near, h, here, here, weight, near_rows, far_rows, owner_near)
                o_copy(near, s).start()

    def place(into, k, joined, source):
        padded[0, :GROUP, :] = joined
        padded[1, :GROUP, :] = source
        gap = padded[0].T[total:] - padded[1].T[:total]
        column = 1.0 / (1.0 + jnp.exp2(gap))
        for j in range(GROUP):
            into[k * GROUP + j] = jnp.broadcast_to(column[:, j : j + 1], (total, HD))

    def near_shares(k):
        for step in range(1, chips // 2):

            @pl.when(near_count == step)
            def _():
                lse_wait(k, 0, step)

        own = lse[chip, k]
        joined, source = own, own
        for step in range(1, chips // 2):
            c = (chip + chips - away * step) % chips
            block = lse[c, k]
            joined = joined + jnp.where(near_count >= step, block, 0.0)
            source = jnp.where(owner_side == -step, block, source)
        place(near_share, k, joined, source)

    def shares(k):
        for step in range(chips // 2, chips):

            @pl.when(far_count == step)
            def _():
                lse_wait(k, 1, step)

        joined, source = lse[0, k], lse[0, k]
        for c in range(1, chips):
            block = lse[c, k]
            joined = joined + block
            source = jnp.where(owner_chip == c, block, source)
        place(share, k, joined, source)

    def relay(s):
        o_copy(near, s).wait_recv()
        for h in heads_of(s):
            here = mine[h].astype(F32)
            came = arrived[near, h].astype(F32)
            forward(near, h, here, came, near_share[h], near_rows, far_rows, owner_near)
        o_copy(near, s).start()

    def finish(s):
        o_copy(1 - near, s).wait_recv()
        @pl.when(inside)
        def _():
            for h in heads_of(s):
                here = mine[h].astype(F32)
                far = arrived[1 - near, h].astype(F32)
                forward(1 - near, h, here, far, share[h], far_rows, near_rows, owner_far)
            o_copy(1 - near, s).start()

        for h in heads_of(s):
            here = mine[h].astype(F32)
            far = arrived[1 - near, h].astype(F32)
            close = arrived[near, h].astype(F32)
            x = jnp.where(is_mine, here, jnp.where(owner_near, close, far))
            y = jnp.where(own_rows, suffix_rows(h), jnp.where(near_rows, close, far))
            done = (near_rows & owner_near) | (far_rows & owner_far)
            attn[h] = jnp.where(done, y, y + share[h] * (x - y)).astype(BF16)
        a_copy(s).start()

    def project(block, half, pair):
        left = jnp.concatenate([block[2 * pair], block[2 * pair + 1]], axis=1)
        rows = wbuf[half, pair * 2 * HD : (pair + 1) * 2 * HD, :]
        return jnp.dot(left, rows, preferred_element_type=F32)

    def ready(pair, s):
        first, size = PARCELS[s]
        return first <= 2 * pair + 1 < first + size

    def inner(group, k):
        @pl.when(inside)
        def _():
            for s in group:
                if s == parcels(k)[0]:
                    near_shares(k)
                relay(s)

    for k in range(HALF_G):
        head(k)
        if k >= BEHIND:
            inner(parcels(k - BEHIND), k - BEHIND)

    last = len(PARCELS)
    rest = [(s, k) for k in range(HALF_G - BEHIND, HALF_G) for s in parcels(k)]
    pltpu.make_async_copy(wbuf, wbuf, w_sem.at[0]).wait()

    @pl.when(at_end)
    def _():
        for k in range(HALF_G):
            shares(k)

    def gather(first, stop):
        bounds = (0, *EDGES, PAIRS)
        for batch in range(len(EDGES) + 1):
            if first <= bounds[batch] < stop:
                block = attn_in.at[pl.ds(2 * bounds[batch], 2 * (bounds[batch + 1] - bounds[batch]))]
                remote(block, block, a_send.at[0], a_recv.at[batch], partner).wait_recv()

    def product(block, half, first, stop):
        sums = project(block, half, first)
        for pair in range(first + 1, stop):
            sums = sums + project(block, half, pair)
        return sums

    for s in range(last):
        k = PARCELS[s][0] // GROUP
        if rest:
            inner([rest[0][0]], rest[0][1])
            rest = rest[1:]
        if s == parcels(k)[0]:

            @pl.when(inside)
            def _():
                shares(k)

        finish(s)
        if s in BATCHES:

            @pl.when(at_end)
            def _():
                (own_from, own_to), (other_from, other_to) = BATCHES[s]
                part = product(attn, core, own_from, own_to)
                gather(other_from, other_to)
                part = part + product(attn_in, 1 - core, other_from, other_to)
                acc[...] = part if s == min(BATCHES) else acc[...] + part

    (_, own_at), (_, other_at) = BATCHES[max(BATCHES)]

    @pl.when(inside)
    def _():
        part = product(attn, core, 0, own_at)
        gather(0, other_at)
        acc[...] = part + product(attn_in, 1 - core, 0, other_at)

    total_sum = acc[...] + product(attn, core, own_at, PAIRS)
    gather(other_at, PAIRS - 1)
    total_sum = total_sum + product(attn_in, 1 - core, other_at, PAIRS - 1)
    gather(PAIRS - 1, PAIRS)
    total_sum = total_sum + product(attn_in, 1 - core, PAIRS - 1, PAIRS)
    out_ref[0] = total_sum.astype(BF16)

    s_copy.wait_send()
    t_copy.wait_send()
    for k in range(HALF_G):
        sent = kv[k].at[core]
        remote(sent, sent, kv_send.at[k], kv_recv.at[k], partner).wait_send()
    block = qall.at[:, pl.ds(0, n - 1)]
    remote(block, block, q_send.at[0], q_recv.at[0], partner).wait_send()
    remote(attn, attn, a_send.at[0], a_recv.at[0], partner).wait_send()
    block = lse.at[pl.ds(0, chips - 1)]
    remote(block, block, lse_send.at[0], lse_recv.at[0, 0], partner).wait_send()

    def sent_all(way):
        block = leaving.at[way]
        remote(block, block, o_send.at[way], o_recv.at[way, 0], partner).wait_send()

    sent_all(near)

    @pl.when(inside)
    def _():
        sent_all(1 - near)
def local(n, queries, prompt_cache, owner, prompt_len, suffix_cache, suffix_len, new_kv, out_weight):
    count = queries.shape[1]
    total = n * count
    chips = n // 2
    span = 2 * total
    slen = suffix_cache.shape[2]
    positions = prompt_cache.shape[2]
    width = out_weight.shape[1]
    hbm = pl.BlockSpec(memory_space=pltpu.HBM)
    vmem = pltpu.VMEM
    smem = pltpu.SMEM
    dma = pltpu.SemaphoreType.DMA
    stream = vmem((2, HALF_H, total, HD), BF16)
    chunk = vmem((HALF_H, total, HD), BF16)
    last = len(PARCELS)
    return pl.pallas_call(
        functools.partial(kernel, n),
        out_shape=pltpu.VMEM((1, total, width), BF16),
        in_specs=[hbm] * 8,
        out_specs=pl.BlockSpec(memory_space=pltpu.VMEM),
        scratch_shapes=[
            *[vmem((2, 2, positions, HD), BF16)] * HALF_G,
            vmem((count, slen, 2 * KW), BF16),
            vmem((2, HALF_W, width), BF16),
            smem((1,), jnp.int32),
            smem((1,), jnp.int32),
            smem((1, count), jnp.int32),
            vmem((count, H * HD), BF16),
            vmem((count, 2 * KW), BF16),
            vmem((HALF_G, n, count, GW), BF16),
            vmem((H * count, HD), F32),
            vmem((H * count, HD), F32),
            vmem((2, count, HALF_W), BF16),
            vmem((count, HALF_W), BF16),
            vmem((2 * count, HALF_W), F32),
            vmem((H, span), F32),
            vmem((2, HALF_H, span), F32),
            vmem((HALF_H, span), F32),
            vmem((HALF_H, span), F32),
            vmem((span, HD), F32),
            vmem((2 * count, HD), F32),
            vmem((chips, HALF_G, GROUP, span), F32),
            vmem((2, HD, span), F32),
            vmem((HALF_H, total, HD), F32),
            vmem((HALF_H, total, HD), F32),
            chunk,
            stream,
            stream,
            chunk,
            chunk,
            vmem((total, width), F32),
            dma((5,)),
            dma((count // 2,)),
            dma((HALF_G,)),
            dma((1,)),
            dma((1,)),
            dma((HALF_G,)),
            dma((2,)),
            dma((2,)),
            dma((HALF_G,)),
            dma((HALF_G,)),
            dma((1,)),
            dma((2, HALF_G)),
            dma((2,)),
            dma((2, last)),
            dma((1,)),
            dma((len(EDGES) + 1,)),
        ],
        compiler_params=pltpu.CompilerParams(
            collective_id=0, has_side_effects=True, vmem_limit_bytes=60 * 1024 * 1024
        ),
        name="shared_decode",
    )(owner, prompt_len, suffix_len, queries, new_kv, prompt_cache, suffix_cache, out_weight)


def solution(mesh):
    in_specs = (
        P("prompt", "sample", None),
        P("prompt", "sample", None, None),
        P("prompt"),
        P("prompt"),
        P("prompt", "sample", None, None),
        P("prompt", "sample"),
        P("prompt", "sample", None),
        P(None, "sample"),
    )
    out_specs = P("prompt", None, "sample")
    body = functools.partial(local, mesh.shape["sample"])
    return jax.shard_map(body, mesh=mesh, in_specs=in_specs, out_specs=out_specs, check_vma=False)
```
